256 devices in a mesh: vocab: 256 (over x, y, z, core).
Axes of the slice: x: 4, y: 4, z: 8, core: 2. Of those that a mesh axis runs over, the one named last changes fastest.
Arguments:
- hidden: bfloat16 [2, 256, 3584], P(None, 'vocab'), may hold values from -256 to 256
- head_weight: bfloat16 [3584, 196608], P(None, 'vocab'), may hold values from -1 to 1
- teacher: bfloat16 [2, 256, 196608], P(None, None, 'vocab'), may hold values from 0 to 1
Outputs:
- token_loss: float32 [2, 256], P(None, 'vocab')
- hidden_grad: bfloat16 [2, 256, 3584], P(None, 'vocab')
- head_grad: bfloat16 [3584, 196608], P(None, 'vocab')
The draws below stay inside these ranges and needn't reach their ends.
All inputs are finite; a program needn't handle non-finite values.
Results may differ from the reference program's by a relative error of at most 0.012.
Values may be sent and summed in bfloat16 or wider, within the bound.
A program may use at most 128 MiB of HBM per device.

```python
import math
import jax
import jax.numpy as jnp
from jax import lax

D = 3584
GROUP = 256
GROUPS = 2
VOCAB = 196608


def draw_head_weight(key, part):
    key_base, key_scale = jax.random.split(jax.random.fold_in(key, 11), 2)
    column_scale = jnp.exp(jax.random.uniform(key_scale, (1, VOCAB), minval=math.log(0.3), maxval=math.log(3.0)))
    base = jnp.clip(jax.random.normal(key_base, (D, VOCAB)), -6.0, 6.0)
    weight = base * column_scale / math.sqrt(D)
    return jnp.clip(weight, -1.0, 1.0).astype(jnp.bfloat16)


def draw_hidden(key, part):
    key_base, key_scale = jax.random.split(jax.random.fold_in(key, 13), 2)
    base = jnp.clip(jax.random.normal(key_base, (GROUPS, GROUP, D)), -6.0, 6.0)
    row_scale = jnp.exp(jax.random.uniform(key_scale, (GROUPS, GROUP, 1), minval=math.log(0.05), maxval=math.log(0.5)))
    states = (base * row_scale).reshape(GROUPS * GROUP, D)
    return states.reshape(GROUPS, GROUP, D).astype(jnp.bfloat16)


def draw_teacher(key, part):
    key_raw, key_weight = jax.random.split(jax.random.fold_in(key, 17), 2)
    position = jnp.arange(VOCAB, dtype=jnp.float32) / VOCAB
    raw = 2.0 * jnp.clip(jax.random.normal(key_raw, (GROUPS, GROUP, VOCAB)), -6.0, 6.0)
    log_mean = 2.0
    rising = math.log(3.0)
    shift_value = log_mean + math.log(VOCAB) + math.log((math.exp(rising) - 1.0) / rising)
    token_weight = jax.random.uniform(key_weight, (GROUPS, GROUP, 1), minval=0.5, maxval=1.5)
    probable = token_weight * jnp.exp(raw + rising * position - shift_value)
    return jnp.clip(probable, 0.0, 1.0).astype(jnp.bfloat16)


def setup_inputs(seed: int = 0) -> dict:
    splits = jax.random.split(jax.random.key(seed), 4)
    hidden = draw_hidden(jax.random.fold_in(splits[3], 71), 0)
    head_weight = draw_head_weight(jax.random.fold_in(splits[3], 71), 0)
    teacher = draw_teacher(jax.random.fold_in(splits[3], 71), 0)
    return {"hidden": hidden, "head_weight": head_weight, "teacher": teacher}


def reference(hidden, head_weight, teacher):
    loss_list = []
    hidden_list = []
    weight_grad = jnp.zeros(head_weight.shape, jnp.bfloat16)
    for group_index in range(GROUPS):
        logit_block = jnp.dot(hidden[group_index], head_weight, preferred_element_type=jnp.float32)
        target_wide = teacher[group_index].astype(jnp.float32)
        peak_logit = jnp.max(logit_block, axis=-1, keepdims=True)
        exp_total = jnp.sum(jnp.exp(logit_block - peak_logit), axis=-1, keepdims=True)
        log_norm = peak_logit + jnp.log(exp_total)
        teacher_mass = jnp.sum(target_wide, axis=-1, keepdims=True)
        cross_term = jnp.sum(target_wide * logit_block, axis=-1, keepdims=True)
        loss_list.append((teacher_mass * log_norm - cross_term)[:, 0])
        logit_grad = (teacher_mass * jnp.exp(logit_block - log_norm) - target_wide).astype(jnp.bfloat16)
        hidden_list.append(jnp.dot(logit_grad, head_weight.T, preferred_element_type=jnp.float32).astype(jnp.bfloat16))
        product_term = lax.dot_general(hidden[group_index], logit_grad, (((0,), (0,)), ((), ())), preferred_element_type=jnp.float32)
        weight_grad = (weight_grad.astype(jnp.float32) + product_term).astype(jnp.bfloat16)
    return (jnp.stack(loss_list), jnp.stack(hidden_list), weight_grad)
```

```python
import jax
import jax.numpy as jnp
from jax import lax
from jax.experimental import pallas as pl
from jax.experimental.pallas import tpu as pltpu
from jax.sharding import Mesh
from jax.sharding import PartitionSpec as P

AXES = ("x", "y", "z", "c")
NX, NY, NZ, NC = 4, 4, 8, 2
LINE = NZ * NC
PLANE = NX * NY
BF16, F32 = jnp.bfloat16, jnp.float32
MESH = pl.DeviceIdType.MESH
RING = (2, 1, 3, 0)
FAR_LINE = (8, 7, 9, 6, 10, 5, 11, 4, 12, 3, 13, 2, 14, 1, 15)


def main_kernel(
    hidden_ref, head_ref, teacher_ref, loss_ref, hgrad_ref, hid_out, grad_out,
    own, landed, spread, hid, head, teach, logit, grad, acc, half_out, half_in,
    ring_out, ring_in, side_out, side_in, line_out, line_in,
    stat_out, stat_line, stat_mid, stat_plane, stat_all,
    local_sem, p1_s, p1_r, d1_s, d1_r, d2_s, d2_r, pair_s, pair_r,
    sl_s, sl_r, sp_s, sp_r, sa_s, sa_r, hp_s, hp_r, rr_s, rr_r, rd_s, rd_r, zl_s, zl_r,
):
    me = {a: lax.axis_index(a) for a in AXES}
    core = me["c"]
    other = 1 - core
    sign = 1 - 2 * core
    rank = me["z"] * NC + core
    place = me["x"] * NY + me["y"]
    width = hidden_ref.shape[1]
    half = width // 2
    quarter = half // 2
    groups = hidden_ref.shape[0]
    started = []

    def send(src, dst, ssem, rsem, where):
        copy = pltpu.make_async_remote_copy(
            src_ref=src, dst_ref=dst, send_sem=ssem, recv_sem=rsem, device_id=where, device_id_type=MESH
        )
        copy.start()
        started.append(copy)
        return copy

    def line_peer(step):
        peer = lax.rem(rank + step, LINE)
        return peer, {"z": peer // NC, "c": lax.rem(peer, NC)}

    def plane_peer(step):
        peer = lax.rem(place + step, PLANE)
        return peer, {"x": peer // NY, "y": lax.rem(peer, NY)}

    def along(axis, step):
        return lax.rem(me[axis] + step + 4, 4)

    local = [
        pltpu.make_async_copy(head_ref, head, local_sem.at[0]),
        pltpu.make_async_copy(teacher_ref, teach, local_sem.at[1]),
    ]
    for copy in local:
        copy.start()

    barrier = pltpu.get_barrier_semaphore()
    for step in range(1, LINE):
        _, where = line_peer(step)
        pl.semaphore_signal(barrier, inc=1, device_id=where, device_id_type=MESH)
    for step in range(1, PLANE):
        _, where = plane_peer(step)
        pl.semaphore_signal(barrier, inc=1, device_id=where, device_id_type=MESH)

    mine = hidden_ref[...]
    for c in range(NC):
        own[c] = mine[:, c * half : (c + 1) * half]
    landed[rank] = own[core]
    pl.semaphore_wait(barrier, LINE - 1 + PLANE - 1)

    line = {}
    for step in FAR_LINE:
        peer, where = line_peer(step)
        line[step] = send(own.at[where["c"]], landed.at[rank], p1_s.at[step], p1_r.at[step], where)
    for step in FAR_LINE:
        line[step].wait_recv()
    for j in range(LINE):
        pair = landed[j].astype(F32)
        for g in range(groups):
            spread[g, j : j + 1] = pair[g : g + 1]
    for k in range(2):
        hid[2 * core + k, :, me["x"], me["y"]] = spread[:, :, k * quarter : (k + 1) * quarter].astype(BF16)

    first, second = ("x", "y"), ("y", "x")

    def block(k, i1, i2):
        i = (i1, i2) if k == 0 else (i2, i1)
        return hid.at[2 * core + k, :, i[0], i[1]]

    direct, ring, pair = {}, {}, {}
    for k in range(2):
        mine = block(k, me[first[k]], me[second[k]])
        for step in (2, 1, 3):
            direct[k, step] = send(
                mine, mine, d1_s.at[k, step], d1_r.at[k, step], {first[k]: along(first[k], step)}
            )
    for n, r in enumerate((0, 1, 3, 2)):
        for k in range(2):
            if r:
                direct[k, r].wait_recv()
            column = block(k, along(first[k], -r), me[second[k]])
            for d in range(2):
                ring[k, r, d] = send(
                    column, column, d2_s.at[k, r, d], d2_r.at[k, r, d], {second[k]: along(second[k], sign * (1 - 2 * d))}
                )
    for r in (0, 1, 3, 2):
        for k in range(2):
            ring[k, r, 0].wait_recv()
            column = block(k, along(first[k], -r), along(second[k], -sign))
            ring[k, r, 2] = send(
                column, column, d2_s.at[k, r, 2], d2_r.at[k, r, 2], {second[k]: along(second[k], sign)}
            )
    for r in (0, 1, 3, 2):
        for k in range(2):
            ring[k, r, 1].wait_recv()
            ring[k, r, 2].wait_recv()
            i1 = along(first[k], -r)
            column = hid.at[2 * core + k, :, i1] if k == 0 else hid.at[2 * core + k, :, :, i1]
            pair[k, r] = send(column, column, pair_s.at[k, r], pair_r.at[k, r], {"c": other})
    for copy in local:
        copy.wait()

    rows = groups * PLANE * LINE
    blocks = logit.shape[1] // 256

    def add_quarter(q, fresh):
        rows_q = hid[q].reshape(rows, quarter)
        for n in range(blocks):
            cols = slice(n * 256, (n + 1) * 256)
            term = jnp.dot(rows_q, head[q, :, cols], preferred_element_type=F32)
            logit[:, cols] = term if fresh else logit[:, cols] + term

    add_quarter(2 * core, True)
    add_quarter(2 * core + 1, False)
    for k in range(2):
        for r in (0, 1, 3, 2):
            pair[k, r].wait_recv()
        add_quarter(2 * other + k, False)
    keep_hid = pltpu.make_async_copy(hid, hid_out, local_sem.at[2])
    keep_hid.start()

    per = rows // groups
    lane = lax.broadcasted_iota(jnp.int32, (per, 128), 1)
    for g in range(groups):
        part = logit[g * per : (g + 1) * per]
        wide = teach[g].astype(F32)
        peak = jnp.max(part, axis=1, keepdims=True)
        total = jnp.sum(jnp.exp(part - peak), axis=1, keepdims=True)
        mass = jnp.sum(wide, axis=1, keepdims=True)
        cross = jnp.sum(wide * part, axis=1, keepdims=True)
        packed = jnp.where(lane == 0, peak, jnp.where(lane == 1, total, jnp.where(lane == 2, mass, cross)))
        stat_out[g] = packed.T[:4]
    stat_line[rank] = stat_out[core]
    line = {}
    for step in FAR_LINE:
        peer, where = line_peer(step)
        line[step] = send(stat_out.at[where["c"]], stat_line.at[rank], sl_s.at[step], sl_r.at[step], where)
    for step in FAR_LINE:
        line[step].wait_recv()

    def combined(ref, count):
        every = [ref[j] for j in range(count)]
        peak = every[0][0:1]
        for one in every[1:]:
            peak = jnp.maximum(peak, one[0:1])
        total = sum(one[1:2] * jnp.exp(one[0:1] - peak) for one in every)
        mass = sum(one[2:3] for one in every)
        cross = sum(one[3:4] for one in every)
        return peak, total, mass, cross

    stat_mid[...] = jnp.concatenate(combined(stat_line, LINE), axis=0)
    stat_plane[place] = stat_mid[...]
    plane = []
    for step in range(1, PLANE):
        _, where = plane_peer(step)
        plane.append(send(stat_mid, stat_plane.at[place], sp_s.at[step], sp_r.at[step], where))
    for copy in plane:
        copy.wait_recv()
    peak, total, mass, cross = combined(stat_plane, PLANE)
    norm = peak + jnp.log(total)
    stat_all[core] = jnp.concatenate([norm, mass, mass * norm - cross, peak], axis=0)
    swap = send(stat_all.at[core], stat_all.at[core], sa_s.at[0], sa_r.at[0], {"c": other})
    swap.wait_recv()

    token = lax.broadcasted_iota(jnp.int32, (1, per), 1)
    for g in range(groups):
        final = stat_all[g]
        loss = jnp.sum(jnp.where(token == place * LINE + rank, final[2:3], 0.0), axis=1, keepdims=True)
        loss_ref[g : g + 1] = loss
        tall = jnp.concatenate([final, jnp.zeros((124, per), F32)], axis=0).T
        part = logit[g * per : (g + 1) * per]
        grad[g] = (tall[:, 1:2] * jnp.exp(part - tall[:, 0:1]) - teach[g].astype(F32)).astype(BF16)
    keep_grad = pltpu.make_async_copy(grad, grad_out, local_sem.at[3])
    keep_grad.start()

    shape = (groups, NX, NY, LINE, quarter)

    def share(q):
        return lax.dot_general(
            grad[...].reshape(rows, -1), head[q], (((1,), (1,)), ((), ())), preferred_element_type=F32
        ).reshape(shape)

    over = []
    for k in range(2):
        half_out[k] = share(2 * other + k).astype(BF16)
        over.append(send(half_out.at[k], half_in.at[k], hp_s.at[k], hp_r.at[k], {"c": other}))
    for k in range(2):
        acc[k] = share(2 * core + k)

    def mine_at(k, i1, i2):
        i = (i1, i2) if k == 0 else (i2, i1)
        return acc[k, :, i[0], i[1]] + half_in[k, :, i[0], i[1]].astype(F32)

    ring, side = {}, {}

    def push(k, r, d, value, step):
        ring_out[k, r, d] = value.astype(BF16)
        ring[k, r, d] = send(
            ring_out.at[k, r, d], ring_in.at[k, r, d], rr_s.at[k, r, d], rr_r.at[k, r, d],
            {second[k]: along(second[k], step)},
        )

    for k in range(2):
        over[k].wait_recv()
        for r in RING:
            i1 = along(first[k], r)
            push(k, r, 0, mine_at(k, i1, along(second[k], 2)), sign)
            push(k, r, 1, mine_at(k, i1, along(second[k], -sign)), -sign)
    for r in RING:
        for k in range(2):
            i1 = along(first[k], r)
            ring[k, r, 0].wait_recv()
            push(k, r, 2, mine_at(k, i1, along(second[k], sign)) + ring_in[k, r, 0].astype(F32), sign)
    kept = {}
    for r in RING:
        for k in range(2):
            i1 = along(first[k], r)
            ring[k, r, 1].wait_recv()
            ring[k, r, 2].wait_recv()
            total = mine_at(k, i1, me[second[k]]) + ring_in[k, r, 1].astype(F32) + ring_in[k, r, 2].astype(F32)
            if r:
                side_out[k, r] = total.astype(BF16)
                side[k, r] = send(
                    side_out.at[k, r], side_in.at[k, r], rd_s.at[k, r], rd_r.at[k, r], {first[k]: i1}
                )
            else:
                kept[k] = total

    for k in range(2):
        for r in (2, 1, 3):
            side[k, r].wait_recv()
            kept[k] = kept[k] + side_in[k, r].astype(F32)
        spread[:, :, k * quarter : (k + 1) * quarter] = kept[k]
    for j in range(LINE):
        line_out[j] = jnp.concatenate([spread[g, j : j + 1] for g in range(groups)], axis=0).astype(BF16)
    line_in[core, me["z"]] = line_out[rank]
    line = {}
    for step in FAR_LINE:
        peer, where = line_peer(step)
        line[step] = send(line_out.at[peer], line_in.at[core, me["z"]], zl_s.at[step], zl_r.at[step], where)
    for step in FAR_LINE:
        line[step].wait_recv()
    for c in range(NC):
        total = line_in[c, 0].astype(F32)
        for z in range(1, NZ):
            total = total + line_in[c, z].astype(F32)
        hgrad_ref[:, c * half : (c + 1) * half] = total.astype(BF16)

    for copy in started:
        copy.wait_send()
    keep_hid.wait()
    keep_grad.wait()


def head_kernel(hid_ref, grad_ref, out_ref):
    rows = grad_ref.shape[0] * grad_ref.shape[1]
    states = hid_ref[0].reshape(rows, hid_ref.shape[-1])
    out_ref[...] = lax.dot_general(
        states, grad_ref[...].reshape(rows, -1), (((0,), (0,)), ((), ())), preferred_element_type=F32
    ).astype(BF16)


def shards(hidden, head_weight, teacher):
    groups, _, width = hidden.shape
    columns = head_weight.shape[1]
    tokens = teacher.shape[1]
    half, quarter = width // 2, width // 4
    plane = (groups, NX, NY, LINE, quarter)
    block = (groups, LINE, quarter)
    dma = pltpu.SemaphoreType.DMA
    vmem = pl.BlockSpec(memory_space=pltpu.VMEM)
    any_space = pl.BlockSpec(memory_space=pl.ANY)
    loss, hgrad, hid, grad = pl.pallas_call(
        main_kernel,
        name="gather_loss_reduce",
        out_shape=(
            jax.ShapeDtypeStruct((groups, 1), F32),
            jax.ShapeDtypeStruct((groups, width), BF16),
            jax.ShapeDtypeStruct((4, *plane), BF16),
            jax.ShapeDtypeStruct((groups, tokens, columns), BF16),
        ),
        in_specs=[vmem, any_space, any_space],
        out_specs=(vmem, vmem, any_space, any_space),
        scratch_shapes=[
            pltpu.VMEM((NC, groups, half), BF16),
            pltpu.VMEM((LINE, groups, half), BF16),
            pltpu.VMEM((groups, LINE, half), F32),
            pltpu.VMEM((4, *plane), BF16),
            pltpu.VMEM((4, quarter, columns), BF16),
            pltpu.VMEM((groups, tokens, columns), BF16),
            pltpu.VMEM((groups * tokens, columns), F32),
            pltpu.VMEM((groups, tokens, columns), BF16),
            pltpu.VMEM((2, *plane), F32),
            pltpu.VMEM((2, *plane), BF16),
            pltpu.VMEM((2, *plane), BF16),
            pltpu.VMEM((2, 4, 3, *block), BF16),
            pltpu.VMEM((2, 4, 3, *block), BF16),
            pltpu.VMEM((2, 4, *block), BF16),
            pltpu.VMEM((2, 4, *block), BF16),
            pltpu.VMEM((LINE, groups, half), BF16),
            pltpu.VMEM((NC, NZ, groups, half), BF16),
            pltpu.VMEM((groups, 4, tokens), F32),
            pltpu.VMEM((LINE, 4, tokens), F32),
            pltpu.VMEM((4, tokens), F32),
            pltpu.VMEM((PLANE, 4, tokens), F32),
            pltpu.VMEM((groups, 4, tokens), F32),
            dma((4,)),
            dma((LINE,)), dma((LINE,)),
            dma((2, 4)), dma((2, 4)),
            dma((2, 4, 3)), dma((2, 4, 3)),
            dma((2, 4)), dma((2, 4)),
            dma((LINE,)), dma((LINE,)),
            dma((PLANE,)), dma((PLANE,)),
            dma((1,)), dma((1,)),
            dma((2,)), dma((2,)),
            dma((2, 4, 3)), dma((2, 4, 3)),
            dma((2, 4)), dma((2, 4)),
            dma((LINE,)), dma((LINE,)),
        ],
        compiler_params=pltpu.CompilerParams(
            collective_id=0, has_side_effects=True, vmem_limit_bytes=56 * 1024 * 1024
        ),
    )(hidden.reshape(groups, width), head_weight.reshape(4, quarter, columns), teacher)
    head_grad = pl.pallas_call(
        head_kernel,
        name="head_gradient",
        grid=(4,),
        out_shape=jax.ShapeDtypeStruct((width, columns), BF16),
        in_specs=[
            pl.BlockSpec((1, *plane), lambda i: (i, 0, 0, 0, 0, 0)),
            pl.BlockSpec((groups, tokens, columns), lambda i: (0, 0, 0)),
        ],
        out_specs=pl.BlockSpec((quarter, columns), lambda i: (i, 0)),
    )(hid, grad)
    return (loss, hgrad.reshape(groups, 1, width), head_grad)


def solution(mesh):
    split = Mesh(mesh.devices.reshape(NX, NY, NZ, NC), AXES)
    return jax.shard_map(
        shards,
        mesh=split,
        in_specs=(P(None, AXES, None), P(None, AXES), P(None, None, AXES)),
        out_specs=(P(None, AXES), P(None, AXES, None), P(None, AXES)),
        check_vma=False,
    )
```

```python
import jax
import jax.numpy as jnp
from jax import lax
from jax.experimental import pallas as pl
from jax.experimental.pallas import tpu as pltpu
from jax.sharding import Mesh
from jax.sharding import PartitionSpec as P

AXES = ("x", "y", "z", "c")
NX, NY, NZ, NC = 4, 4, 8, 2
LINE = NZ * NC
PLANE = NX * NY
BF16, F32 = jnp.bfloat16, jnp.float32
MESH = pl.DeviceIdType.MESH
RING = (2, 1, 3, 0)
FAR_LINE = (8, 7, 9, 6, 10, 5, 11, 4, 12, 3, 13, 2, 14, 1, 15)


def main_kernel(
    hidden_ref, head_ref, teacher_ref, loss_ref, hgrad_ref, head_grad_ref,
    own, landed, spread, hid, head, teach, logit, grad, acc, half_out, half_in,
    ring_out, ring_in, side_out, side_in, line_out, line_in,
    stat_out, stat_line, stat_mid, stat_plane, stat_all,
    local_sem, p1_s, p1_r, d1_s, d1_r, d2_s, d2_r, pair_s, pair_r,
    sl_s, sl_r, sp_s, sp_r, sa_s, sa_r, hp_s, hp_r, rr_s, rr_r, rd_s, rd_r, zl_s, zl_r,
):
    me = {a: lax.axis_index(a) for a in AXES}
    core = me["c"]
    other = 1 - core
    sign = 1 - 2 * core
    rank = me["z"] * NC + core
    place = me["x"] * NY + me["y"]
    width = hidden_ref.shape[1]
    half = width // 2
    quarter = half // 2
    groups = hidden_ref.shape[0]
    started = []

    def send(src, dst, ssem, rsem, where):
        copy = pltpu.make_async_remote_copy(
            src_ref=src, dst_ref=dst, send_sem=ssem, recv_sem=rsem, device_id=where, device_id_type=MESH
        )
        copy.start()
        started.append(copy)
        return copy

    def line_peer(step):
        peer = lax.rem(rank + step, LINE)
        return peer, {"z": peer // NC, "c": lax.rem(peer, NC)}

    def plane_peer(step):
        peer = lax.rem(place + step, PLANE)
        return peer, {"x": peer // NY, "y": lax.rem(peer, NY)}

    def along(axis, step):
        return lax.rem(me[axis] + step + 4, 4)

    local = [
        pltpu.make_async_copy(head_ref, head, local_sem.at[0]),
        pltpu.make_async_copy(teacher_ref, teach, local_sem.at[1]),
    ]
    for copy in local:
        copy.start()

    barrier = pltpu.get_barrier_semaphore()
    for step in range(1, LINE):
        _, where = line_peer(step)
        pl.semaphore_signal(barrier, inc=1, device_id=where, device_id_type=MESH)
    for step in range(1, PLANE):
        _, where = plane_peer(step)
        pl.semaphore_signal(barrier, inc=1, device_id=where, device_id_type=MESH)

    mine = hidden_ref[...]
    for c in range(NC):
        own[c] = mine[:, c * half : (c + 1) * half]
    landed[rank] = own[core]
    pl.semaphore_wait(barrier, LINE - 1 + PLANE - 1)

    line = {}
    for step in FAR_LINE:
        peer, where = line_peer(step)
        line[step] = send(own.at[where["c"]], landed.at[rank], p1_s.at[step], p1_r.at[step], where)
    for step in FAR_LINE:
        line[step].wait_recv()
    for j in range(LINE):
        pair = landed[j].astype(F32)
        for g in range(groups):
            spread[g, j : j + 1] = pair[g : g + 1]
    for k in range(2):
        hid[2 * core + k, :, me["x"], me["y"]] = spread[:, :, k * quarter : (k + 1) * quarter].astype(BF16)

    first, second = ("x", "y"), ("y", "x")

    def block(k, i1, i2):
        i = (i1, i2) if k == 0 else (i2, i1)
        return hid.at[2 * core + k, :, i[0], i[1]]

    direct, ring, pair = {}, {}, {}
    for k in range(2):
        mine = block(k, me[first[k]], me[second[k]])
        for step in (2, 1, 3):
            direct[k, step] = send(
                mine, mine, d1_s.at[k, step], d1_r.at[k, step], {first[k]: along(first[k], step)}
            )
    for n, r in enumerate((0, 1, 3, 2)):
        for k in range(2):
            if r:
                direct[k, r].wait_recv()
            column = block(k, along(first[k], -r), me[second[k]])
            for d in range(2):
                ring[k, r, d] = send(
                    column, column, d2_s.at[k, r, d], d2_r.at[k, r, d], {second[k]: along(second[k], sign * (1 - 2 * d))}
                )
    for r in (0, 1, 3, 2):
        for k in range(2):
            ring[k, r, 0].wait_recv()
            column = block(k, along(first[k], -r), along(second[k], -sign))
            ring[k, r, 2] = send(
                column, column, d2_s.at[k, r, 2], d2_r.at[k, r, 2], {second[k]: along(second[k], sign)}
            )
    for r in (0, 1, 3, 2):
        for k in range(2):
            ring[k, r, 1].wait_recv()
            ring[k, r, 2].wait_recv()
            i1 = along(first[k], -r)
            column = hid.at[2 * core + k, :, i1] if k == 0 else hid.at[2 * core + k, :, :, i1]
            pair[k, r] = send(column, column, pair_s.at[k, r], pair_r.at[k, r], {"c": other})
    for copy in local:
        copy.wait()

    rows = groups * PLANE * LINE
    blocks = logit.shape[1] // 256

    def add_quarter(q, fresh):
        rows_q = hid[q].reshape(rows, quarter)
        for n in range(blocks):
            cols = slice(n * 256, (n + 1) * 256)
            term = jnp.dot(rows_q, head[q, :, cols], preferred_element_type=F32)
            logit[:, cols] = term if fresh else logit[:, cols] + term

    add_quarter(2 * core, True)
    add_quarter(2 * core + 1, False)
    for k in range(2):
        for r in (0, 1, 3, 2):
            pair[k, r].wait_recv()
        add_quarter(2 * other + k, False)

    per = rows // groups
    lane = lax.broadcasted_iota(jnp.int32, (per, 128), 1)
    for g in range(groups):
        part = logit[g * per : (g + 1) * per]
        wide = teach[g].astype(F32)
        peak = jnp.max(part, axis=1, keepdims=True)
        total = jnp.sum(jnp.exp(part - peak), axis=1, keepdims=True)
        mass = jnp.sum(wide, axis=1, keepdims=True)
        cross = jnp.sum(wide * part, axis=1, keepdims=True)
        packed = jnp.where(lane == 0, peak, jnp.where(lane == 1, total, jnp.where(lane == 2, mass, cross)))
        stat_out[g] = packed.T[:4]
    stat_line[rank] = stat_out[core]
    line = {}
    for step in FAR_LINE:
        peer, where = line_peer(step)
        line[step] = send(stat_out.at[where["c"]], stat_line.at[rank], sl_s.at[step], sl_r.at[step], where)
    for step in FAR_LINE:
        line[step].wait_recv()

    def combined(ref, count):
        every = [ref[j] for j in range(count)]
        peak = every[0][0:1]
        for one in every[1:]:
            peak = jnp.maximum(peak, one[0:1])
        total = sum(one[1:2] * jnp.exp(one[0:1] - peak) for one in every)
        mass = sum(one[2:3] for one in every)
        cross = sum(one[3:4] for one in every)
        return peak, total, mass, cross

    stat_mid[...] = jnp.concatenate(combined(stat_line, LINE), axis=0)
    stat_plane[place] = stat_mid[...]
    plane = []
    for step in range(1, PLANE):
        _, where = plane_peer(step)
        plane.append(send(stat_mid, stat_plane.at[place], sp_s.at[step], sp_r.at[step], where))
    for copy in plane:
        copy.wait_recv()
    peak, total, mass, cross = combined(stat_plane, PLANE)
    norm = peak + jnp.log(total)
    stat_all[core] = jnp.concatenate([norm, mass, mass * norm - cross, peak], axis=0)
    swap = send(stat_all.at[core], stat_all.at[core], sa_s.at[0], sa_r.at[0], {"c": other})
    swap.wait_recv()

    token = lax.broadcasted_iota(jnp.int32, (1, per), 1)
    for g in range(groups):
        final = stat_all[g]
        loss = jnp.sum(jnp.where(token == place * LINE + rank, final[2:3], 0.0), axis=1, keepdims=True)
        loss_ref[:, g : g + 1] = loss
        tall = jnp.concatenate([final, jnp.zeros((124, per), F32)], axis=0).T
        part = logit[g * per : (g + 1) * per]
        grad[g] = (tall[:, 1:2] * jnp.exp(part - tall[:, 0:1]) - teach[g].astype(F32)).astype(BF16)

    shape = (groups, NX, NY, LINE, quarter)

    def share(q):
        return lax.dot_general(
            grad[...].reshape(rows, -1), head[q], (((1,), (1,)), ((), ())), preferred_element_type=F32
        ).reshape(shape)

    over = []
    for k in range(2):
        half_out[k] = share(2 * other + k).astype(BF16)
        over.append(send(half_out.at[k], half_in.at[k], hp_s.at[k], hp_r.at[k], {"c": other}))
    for k in range(2):
        acc[k] = share(2 * core + k)

    def mine_at(k, i1, i2):
        i = (i1, i2) if k == 0 else (i2, i1)
        return acc[k, :, i[0], i[1]] + half_in[k, :, i[0], i[1]].astype(F32)

    ring, side = {}, {}

    def head_gradient(q):
        head_grad_ref[q * quarter : (q + 1) * quarter] = lax.dot_general(
            hid[q].reshape(rows, quarter), grad[...].reshape(rows, -1), (((0,), (0,)), ((), ())),
            preferred_element_type=F32,
        ).astype(BF16)

    def push(k, r, d, value, step):
        ring_out[k, r, d] = value.astype(BF16)
        ring[k, r, d] = send(
            ring_out.at[k, r, d], ring_in.at[k, r, d], rr_s.at[k, r, d], rr_r.at[k, r, d],
            {second[k]: along(second[k], step)},
        )

    for k in range(2):
        over[k].wait_recv()
        for r in RING:
            i1 = along(first[k], r)
            push(k, r, 0, mine_at(k, i1, along(second[k], 2)), sign)
            push(k, r, 1, mine_at(k, i1, along(second[k], -sign)), -sign)
    head_gradient(0)
    head_gradient(1)
    for r in RING:
        for k in range(2):
            i1 = along(first[k], r)
            ring[k, r, 0].wait_recv()
            push(k, r, 2, mine_at(k, i1, along(second[k], sign)) + ring_in[k, r, 0].astype(F32), sign)
    head_gradient(2)
    kept = {}
    for r in RING:
        for k in range(2):
            i1 = along(first[k], r)
            ring[k, r, 1].wait_recv()
            ring[k, r, 2].wait_recv()
            total = mine_at(k, i1, me[second[k]]) + ring_in[k, r, 1].astype(F32) + ring_in[k, r, 2].astype(F32)
            if r:
                side_out[k, r] = total.astype(BF16)
                side[k, r] = send(
                    side_out.at[k, r], side_in.at[k, r], rd_s.at[k, r], rd_r.at[k, r], {first[k]: i1}
                )
            else:
                kept[k] = total

    head_gradient(3)
    for k in range(2):
        for r in (2, 1, 3):
            side[k, r].wait_recv()
            kept[k] = kept[k] + side_in[k, r].astype(F32)
        spread[:, :, k * quarter : (k + 1) * quarter] = kept[k]
    for j in range(LINE):
        line_out[j] = jnp.concatenate([spread[g, j : j + 1] for g in range(groups)], axis=0).astype(BF16)
    line_in[core, me["z"]] = line_out[rank]
    line = {}
    for step in FAR_LINE:
        peer, where = line_peer(step)
        line[step] = send(line_out.at[peer], line_in.at[core, me["z"]], zl_s.at[step], zl_r.at[step], where)
    for step in FAR_LINE:
        line[step].wait_recv()
    for c in range(NC):
        total = line_in[c, 0].astype(F32)
        for z in range(1, NZ):
            total = total + line_in[c, z].astype(F32)
        hgrad_ref[:, c * half : (c + 1) * half] = total.astype(BF16)

    for copy in started:
        copy.wait_send()


def shards(hidden, head_weight, teacher):
    groups, _, width = hidden.shape
    columns = head_weight.shape[1]
    tokens = teacher.shape[1]
    half, quarter = width // 2, width // 4
    plane = (groups, NX, NY, LINE, quarter)
    block = (groups, LINE, quarter)
    dma = pltpu.SemaphoreType.DMA
    vmem = pl.BlockSpec(memory_space=pltpu.VMEM)
    any_space = pl.BlockSpec(memory_space=pl.ANY)
    loss, hgrad, head_grad = pl.pallas_call(
        main_kernel,
        name="gather_loss_reduce",
        out_shape=(
            pltpu.VMEM((1, groups), F32),
            pltpu.VMEM((groups, width), BF16),
            pltpu.VMEM((width, columns), BF16),
        ),
        in_specs=[vmem, any_space, any_space],
        out_specs=(vmem, vmem, vmem),
        scratch_shapes=[
            pltpu.VMEM((NC, groups, half), BF16),
            pltpu.VMEM((LINE, groups, half), BF16),
            pltpu.VMEM((groups, LINE, half), F32),
            pltpu.VMEM((4, *plane), BF16),
            pltpu.VMEM((4, quarter, columns), BF16),
            pltpu.VMEM((groups, tokens, columns), BF16),
            pltpu.VMEM((groups * tokens, columns), F32),
            pltpu.VMEM((groups, tokens, columns), BF16),
            pltpu.VMEM((2, *plane), F32),
            pltpu.VMEM((2, *plane), BF16),
            pltpu.VMEM((2, *plane), BF16),
            pltpu.VMEM((2, 4, 3, *block), BF16),
            pltpu.VMEM((2, 4, 3, *block), BF16),
            pltpu.VMEM((2, 4, *block), BF16),
            pltpu.VMEM((2, 4, *block), BF16),
            pltpu.VMEM((LINE, groups, half), BF16),
            pltpu.VMEM((NC, NZ, groups, half), BF16),
            pltpu.VMEM((groups, 4, tokens), F32),
            pltpu.VMEM((LINE, 4, tokens), F32),
            pltpu.VMEM((4, tokens), F32),
            pltpu.VMEM((PLANE, 4, tokens), F32),
            pltpu.VMEM((groups, 4, tokens), F32),
            dma((4,)),
            dma((LINE,)), dma((LINE,)),
            dma((2, 4)), dma((2, 4)),
            dma((2, 4, 3)), dma((2, 4, 3)),
            dma((2, 4)), dma((2, 4)),
            dma((LINE,)), dma((LINE,)),
            dma((PLANE,)), dma((PLANE,)),
            dma((1,)), dma((1,)),
            dma((2,)), dma((2,)),
            dma((2, 4, 3)), dma((2, 4, 3)),
            dma((2, 4)), dma((2, 4)),
            dma((LINE,)), dma((LINE,)),
        ],
        compiler_params=pltpu.CompilerParams(
            collective_id=0, has_side_effects=True, vmem_limit_bytes=50 * 1024 * 1024
        ),
    )(hidden.reshape(groups, width), head_weight.reshape(4, quarter, columns), teacher)
    return (loss.reshape(groups, 1), hgrad.reshape(groups, 1, width), head_grad)


def solution(mesh):
    split = Mesh(mesh.devices.reshape(NX, NY, NZ, NC), AXES)
    return jax.shard_map(
        shards,
        mesh=split,
        in_specs=(P(None, AXES, None), P(None, AXES), P(None, None, AXES)),
        out_specs=(P(None, AXES), P(None, AXES, None), P(None, AXES)),
        check_vma=False,
    )
```

```python
import jax
import jax.numpy as jnp
from jax import lax
from jax.experimental import pallas as pl
from jax.experimental.pallas import tpu as pltpu
from jax.sharding import Mesh
from jax.sharding import PartitionSpec as P

AXES = ("x", "y", "z", "c")
NX, NY, NZ, NC = 4, 4, 8, 2
LINE = NZ * NC
PLANE = NX * NY
BF16, F32 = jnp.bfloat16, jnp.float32
MESH = pl.DeviceIdType.MESH
RING = (2, 1, 3, 0)
FAR_PLANE = (10, 5, 7, 15, 13, 8, 2, 9, 11, 14, 6, 3, 1, 12, 4)
FAR_LINE = (8, 7, 9, 6, 10, 5, 11, 4, 12, 3, 13, 2, 14, 1, 15)


def main_kernel(
    hidden_ref, head_ref, teacher_ref, loss_ref, hgrad_ref, head_grad_ref,
    tokens, own, landed, spread, hid, head, teach, logit, grad, raised, raised_share, teach_share, column, half_out, half_in,
    ring_out, ring_in, side_out, side_in, line_out, line_in,
    stat_out, stat_line, stat_mid, stat_plane, stat_all,
    local_sem, sent, p1_r, d1_r, d2_r, pair_r, sl_r, sp_r, hp_r, rr_r, rd_r, zl_r,
):
    me = {a: lax.axis_index(a) for a in AXES}
    core = me["c"]
    other = 1 - core
    sign = 1 - 2 * core
    rank = me["z"] * NC + core
    place = me["x"] * NY + me["y"]
    width = hidden_ref.shape[1]
    half = width // 2
    quarter = half // 2
    groups, per, columns = teacher_ref.shape
    first, second = ("x", "y"), ("y", "x")

    def send(src, dst, ssem, rsem, where):
        copy = pltpu.make_async_remote_copy(
            src_ref=src, dst_ref=dst, send_sem=ssem, recv_sem=rsem, device_id=where, device_id_type=MESH
        )
        copy.start()
        return copy

    def wait_all(ref, sem):
        pltpu.make_async_copy(ref, ref, sem).wait()

    def line_peer(step):
        peer = lax.rem(rank + step, LINE)
        return peer, {"z": peer // NC, "c": lax.rem(peer, NC)}

    def plane_peer(step):
        peer = lax.rem(place + step, PLANE)
        return peer, {"x": peer // NY, "y": lax.rem(peer, NY)}

    def along(axis, step):
        return lax.rem(me[axis] + step + 4, 4)

    def product(ref, g, q):
        return lax.dot_general(
            ref[g], head[q], (((1,), (1,)), ((), ())), preferred_element_type=F32
        ).reshape(NX, NY, LINE, quarter)

    def share_teacher(g, q):
        teach_share[q, g] = product(teach, g, q)

    local = [
        pltpu.make_async_copy(hidden_ref, tokens, local_sem.at[0]),
        pltpu.make_async_copy(head_ref, head, local_sem.at[1]),
        pltpu.make_async_copy(teacher_ref, teach, local_sem.at[2]),
    ]
    for copy in local:
        copy.start()

    barrier = pltpu.get_barrier_semaphore()
    for step in FAR_LINE:
        _, where = line_peer(step)
        pl.semaphore_signal(barrier, inc=1, device_id=where, device_id_type=MESH)
    for step in FAR_PLANE:
        _, where = plane_peer(step)
        for c in (core, other):
            pl.semaphore_signal(barrier, inc=1, device_id={**where, "c": c}, device_id_type=MESH)

    local[0].wait()
    mine = tokens[...]
    for c in range(NC):
        own[c] = mine[:, c * half : (c + 1) * half]
    landed[rank] = own[core]
    pl.semaphore_wait(barrier, LINE - 1 + NC * (PLANE - 1))

    for step in FAR_LINE:
        peer, where = line_peer(step)
        send(own.at[where["c"]], landed.at[rank], sent.at[0], p1_r.at[0], where)
    for copy in local[1:]:
        copy.wait()
    share_teacher(0, 0)
    share_teacher(0, 1)
    share_teacher(0, 2)
    share_teacher(0, 3)
    share_teacher(1, 0)
    wait_all(landed.at[: LINE - 1], p1_r.at[0])
    for j in range(LINE):
        pair = landed[j].astype(F32)
        for g in range(groups):
            spread[g, j : j + 1] = pair[g : g + 1]
    for k in range(2):
        hid[2 * core + k, :, me["x"], me["y"]] = spread[:, :, k * quarter : (k + 1) * quarter].astype(BF16)

    direct, ring = {}, {}
    behind = (0, 1, 3, 2)

    def block(k, g, i1, i2):
        i = (i1, i2) if k == 0 else (i2, i1)
        return hid.at[2 * core + k, g, i[0], i[1]]

    def gather_first(g):
        for k in range(2):
            mine = block(k, g, me[first[k]], me[second[k]])
            for n in (1, 2, 3):
                direct[k, g, n] = send(
                    mine, mine, sent.at[1], d1_r.at[k, g, n], {first[k]: along(first[k], behind[n])}
                )

    def gather_ring(g, order, d):
        for n in order:
            for k in range(2):
                if n and d == 0:
                    direct[k, g, n].wait_recv()
                column = block(k, g, along(first[k], -behind[n]), me[second[k]])
                ring[k, g, n, d] = send(
                    column, column, sent.at[2], d2_r.at[k, g, n, d],
                    {second[k]: along(second[k], sign * (1 - 2 * d))},
                )

    def gather_relay(g):
        for n in range(4):
            for k in range(2):
                ring[k, g, n, 0].wait_recv()
                column = block(k, g, along(first[k], -behind[n]), along(second[k], -sign))
                send(column, column, sent.at[2], d2_r.at[k, g, n, 1], {second[k]: along(second[k], sign)})

    def gather_last(g):
        for n in range(4):
            for k in range(2):
                wait_all(ring_in.at[k, g, n, :2], d2_r.at[k, g, n, 1])
                i1 = along(first[k], -behind[n])
                column = hid.at[2 * core + k, g, i1] if k == 0 else hid.at[2 * core + k, g, :, i1]
                send(column, column, sent.at[3], pair_r.at[k, g], {"c": other})

    def states(q, g):
        return hid[q, g].reshape(per, quarter)

    def add_quarter(g, q, fresh):
        here = slice(g * per, (g + 1) * per)
        for n in range(columns // 256):
            cols = slice(n * 256, (n + 1) * 256)
            term = jnp.dot(states(q, g), head[q, :, cols], preferred_element_type=F32)
            logit[here, cols] = term if fresh else logit[here, cols] + term

    def logits_own(g):
        for k in range(2):
            add_quarter(g, 2 * core + k, k == 0)

    def logits_other():
        for k in range(2):
            for g in range(groups):
                wait_all(hid.at[0, g], pair_r.at[k, g])
            q = 2 * other + k
            every = hid[q].reshape(groups * per, quarter)
            for n in range(columns // 256):
                cols = slice(n * 256, (n + 1) * 256)
                logit[:, cols] += jnp.dot(every, head[q, :, cols], preferred_element_type=F32)

    def statistics():
        lane = lax.broadcasted_iota(jnp.int32, (per, 128), 1)
        for g in range(groups):
            part = logit[g * per : (g + 1) * per]
            wide = teach[g].astype(F32)
            peak = jnp.max(part, axis=1, keepdims=True)
            exponent = jnp.exp(part - peak)
            raised[g] = exponent.astype(BF16)
            total = jnp.sum(exponent, axis=1, keepdims=True)
            mass = jnp.sum(wide, axis=1, keepdims=True)
            cross = jnp.sum(wide * part, axis=1, keepdims=True)
            packed = jnp.where(lane == 0, peak, jnp.where(lane == 1, total, jnp.where(lane == 2, mass, cross)))
            column[g] = jnp.broadcast_to(peak, (per, 128))
            stat_out[g] = packed.T[:4]
        stat_line[rank] = stat_out[core]
        for step in FAR_LINE:
            peer, where = line_peer(step)
            send(stat_out.at[where["c"]], stat_line.at[rank], sent.at[4], sl_r.at[0], where)

    def combined(ref, slots):
        every = [ref[j] for j in slots]
        peak = every[0][0:1]
        for one in every[1:]:
            peak = jnp.maximum(peak, one[0:1])
        total = sum(one[1:2] * jnp.exp(one[0:1] - peak) for one in every)
        mass = sum(one[2:3] for one in every)
        cross = sum(one[3:4] for one in every)
        return peak, total, mass, cross

    def line_done():
        wait_all(stat_line.at[: LINE - 1], sl_r.at[0])
        stat_mid[...] = jnp.concatenate(combined(stat_line, range(LINE)), axis=0)
        slot = core * PLANE + place
        stat_plane[slot] = stat_mid[...]
        for step in (*FAR_PLANE, 0):
            _, where = plane_peer(step)
            for c in (core, other) if step else (other,):
                send(stat_mid, stat_plane.at[slot], sent.at[5], sp_r.at[0], {**where, "c": c})

    def plane_done():
        wait_all(stat_plane.at[: NC * PLANE - 1], sp_r.at[0])
        for g in range(groups):
            peak, total, mass, cross = combined(stat_plane, range(g * PLANE, (g + 1) * PLANE))
            norm = peak + jnp.log(total)
            stat_all[g] = jnp.concatenate([norm, mass, mass * norm - cross, peak], axis=0)

    def scales(g):
        final = stat_all[g]
        token = lax.broadcasted_iota(jnp.int32, (1, per), 1)
        loss = jnp.sum(jnp.where(token == place * LINE + rank, final[2:3], 0.0), axis=1, keepdims=True)
        loss_ref[:, g : g + 1] = loss
        tall = jnp.concatenate([final, jnp.zeros((124, per), F32)], axis=0).T
        peak = column[g, :, 0:1]
        lane = lax.broadcasted_iota(jnp.int32, (per, 128), 1)
        scale = tall[:, 1:2] * jnp.exp(peak - tall[:, 0:1])
        column[g] = jnp.where(lane == 0, tall[:, 0:1], jnp.where(lane == 1, tall[:, 1:2], scale))

    def gradient(g):
        tall = column[g]
        part = logit[g * per : (g + 1) * per]
        grad[g] = (tall[:, 1:2] * jnp.exp(part - tall[:, 0:1]) - teach[g].astype(F32)).astype(BF16)

    over = {}

    def share_raised(g, q):
        raised_share[q, g] = product(raised, g, q)

    def joined(g, q):
        scale = column[g, :, 2:3].reshape(NX, NY, LINE, 1)
        return raised_share[q, g] * scale - teach_share[q, g]

    def share_over(g, k):
        q = 2 * other + k
        half_out[k, g] = joined(g, q).astype(BF16)
        over[k, g] = send(half_out.at[k, g], half_in.at[k, g], sent.at[6], hp_r.at[k, g], {"c": other})

    def share_kept(g, k):
        q = 2 * core + k
        raised_share[q, g] = joined(g, q)

    hop = {}

    def mine_at(k, g, i1, i2):
        i = (i1, i2) if k == 0 else (i2, i1)
        return raised_share[2 * core + k, g, i[0], i[1]] + half_in[k, g, i[0], i[1]].astype(F32)

    def push(k, g, r, d, value, step):
        ring_out[k, g, r, d] = value.astype(BF16)
        hop[k, g, r, d] = send(
            ring_out.at[k, g, r, d], ring_in.at[k, g, r, d], sent.at[7], rr_r.at[k, g, r, min(d, 1)],
            {second[k]: along(second[k], step)},
        )

    def sum_start(g, k, d):
        if d == 0:
            over[k, g].wait_recv()
        for r in RING:
            i1 = along(first[k], r)
            push(k, g, r, d, mine_at(k, g, i1, along(second[k], -sign if d else 2)), -sign if d else sign)

    def sum_relay(g, k):
        for r in RING:
            i1 = along(first[k], r)
            hop[k, g, r, 0].wait_recv()
            carried = ring_in[k, g, r, 0].astype(F32)
            push(k, g, r, 2, mine_at(k, g, i1, along(second[k], sign)) + carried, sign)

    def sum_last(g, k):
        for r in RING:
            i1 = along(first[k], r)
            wait_all(ring_in.at[k, g, r, 1:], rr_r.at[k, g, r, 1])
            total = mine_at(k, g, i1, me[second[k]])
            total = total + ring_in[k, g, r, 1].astype(F32) + ring_in[k, g, r, 2].astype(F32)
            if r:
                side_out[k, g, r] = total.astype(BF16)
                send(side_out.at[k, g, r], side_in.at[k, g, r], sent.at[8], rd_r.at[k, g], {first[k]: i1})
            else:
                spread[g, :, k * quarter : (k + 1) * quarter] = total

    def sum_side(g):
        for k in range(2):
            here = slice(k * quarter, (k + 1) * quarter)
            total = spread[g, :, here]
            wait_all(side_in.at[k, g, 1:], rd_r.at[k, g])
            for r in RING[:3]:
                total = total + side_in[k, g, r].astype(F32)
            spread[g, :, here] = total

    def head_gradient(q):
        head_grad_ref[q * quarter : (q + 1) * quarter] = lax.dot_general(
            hid[q].reshape(groups * per, quarter), grad[...].reshape(groups * per, columns),
            (((0,), (0,)), ((), ())), preferred_element_type=F32,
        ).astype(BF16)

    gather_first(0)
    gather_ring(0, (0,), 0)
    gather_ring(0, (0,), 1)
    gather_first(1)
    share_teacher(1, 1)
    share_teacher(1, 2)
    gather_ring(0, (1, 2, 3), 0)
    gather_ring(0, (1, 2, 3), 1)
    gather_ring(1, (0, 1, 2, 3), 0)
    gather_ring(1, (0, 1, 2, 3), 1)
    share_teacher(1, 3)
    gather_relay(0)
    gather_relay(1)
    gather_last(0)
    logits_own(0)
    gather_last(1)
    logits_own(1)
    logits_other()
    statistics()
    share_raised(0, 2 * other)
    share_raised(0, 2 * core)
    share_raised(0, 2 * other + 1)
    share_raised(0, 2 * core + 1)
    line_done()
    share_raised(1, 2 * other)
    share_raised(1, 2 * core)
    share_raised(1, 2 * other + 1)
    share_raised(1, 2 * core + 1)
    plane_done()
    scales(0)
    share_over(0, 0)
    share_over(0, 1)
    scales(1)
    share_over(1, 0)
    share_over(1, 1)
    share_kept(0, 0)
    sum_start(0, 0, 0)
    share_kept(0, 1)
    sum_start(0, 1, 0)
    share_kept(1, 0)
    sum_start(1, 0, 0)
    share_kept(1, 1)
    sum_start(1, 1, 0)
    sum_start(0, 0, 1)
    sum_start(0, 1, 1)
    sum_relay(0, 0)
    sum_relay(0, 1)
    sum_start(1, 0, 1)
    sum_start(1, 1, 1)
    sum_relay(1, 0)
    sum_relay(1, 1)
    gradient(0)
    gradient(1)
    sum_last(0, 0)
    sum_last(0, 1)
    sum_last(1, 0)
    sum_last(1, 1)
    sum_side(0)
    sum_side(1)
    for j in range(LINE):
        line_out[j] = jnp.concatenate([spread[g, j : j + 1] for g in range(groups)], axis=0).astype(BF16)
    line_in[core, me["z"]] = line_out[rank]
    for step in FAR_LINE:
        peer, where = line_peer(step)
        send(line_out.at[peer], line_in.at[core, me["z"]], sent.at[9], zl_r.at[0], where)
    head_gradient(0)
    head_gradient(1)
    head_gradient(2)
    head_gradient(3)
    wait_all(line_out.at[: LINE - 1], zl_r.at[0])
    for c in range(NC):
        total = line_in[c, 0].astype(F32)
        for z in range(1, NZ):
            total = total + line_in[c, z].astype(F32)
        hgrad_ref[:, c * half : (c + 1) * half] = total.astype(BF16)

    for n, ref in enumerate(
        (
            landed.at[: LINE - 1], ring_in.at[:, :, 0], ring_in, hid.at[:2], stat_line.at[: LINE - 1],
            stat_plane.at[: NC * PLANE - 1], half_out, ring_out, side_out.at[:, :, 1:],
            line_out.at[: LINE - 1],
        )
    ):
        wait_all(ref, sent.at[n])


def place_kernel(loss_in, hgrad_in, head_in, loss_ref, hgrad_ref, head_ref, sem):
    copies = [
        pltpu.make_async_copy(head_in, head_ref, sem.at[0]),
        pltpu.make_async_copy(hgrad_in, hgrad_ref, sem.at[1]),
        pltpu.make_async_copy(loss_in, loss_ref, sem.at[2]),
    ]
    for copy in copies:
        copy.start()
    for copy in copies:
        copy.wait()


def shards(hidden, head_weight, teacher):
    groups, _, width = hidden.shape
    columns = head_weight.shape[1]
    count = teacher.shape[1]
    half, quarter = width // 2, width // 4
    plane = (groups, NX, NY, LINE, quarter)
    block = (LINE, quarter)
    dma = pltpu.SemaphoreType.DMA
    vmem = pl.BlockSpec(memory_space=pltpu.VMEM)
    any_space = pl.BlockSpec(memory_space=pl.ANY)
    results = pl.pallas_call(
        main_kernel,
        name="gather_loss_reduce",
        out_shape=(
            pltpu.VMEM((1, groups), F32),
            pltpu.VMEM((groups, width), BF16),
            pltpu.VMEM((width, columns), BF16),
        ),
        in_specs=[any_space, any_space, any_space],
        out_specs=(vmem, vmem, vmem),
        scratch_shapes=[
            pltpu.VMEM((groups, width), BF16),
            pltpu.VMEM((NC, groups, half), BF16),
            pltpu.VMEM((LINE, groups, half), BF16),
            pltpu.VMEM((groups, LINE, half), F32),
            pltpu.VMEM((4, *plane), BF16),
            pltpu.VMEM((4, quarter, columns), BF16),
            pltpu.VMEM((groups, count, columns), BF16),
            pltpu.VMEM((groups * count, columns), F32),
            pltpu.VMEM((groups, count, columns), BF16),
            pltpu.VMEM((groups, count, columns), BF16),
            pltpu.VMEM((4, *plane), F32),
            pltpu.VMEM((4, *plane), F32),
            pltpu.VMEM((groups, count, 128), F32),
            pltpu.VMEM((2, *plane), BF16),
            pltpu.VMEM((2, *plane), BF16),
            pltpu.VMEM((2, groups, 4, 3, *block), BF16),
            pltpu.VMEM((2, groups, 4, 3, *block), BF16),
            pltpu.VMEM((2, groups, 4, *block), BF16),
            pltpu.VMEM((2, groups, 4, *block), BF16),
            pltpu.VMEM((LINE, groups, half), BF16),
            pltpu.VMEM((NC, NZ, groups, half), BF16),
            pltpu.VMEM((groups, 4, count), F32),
            pltpu.VMEM((LINE, 4, count), F32),
            pltpu.VMEM((4, count), F32),
            pltpu.VMEM((NC * PLANE, 4, count), F32),
            pltpu.VMEM((groups, 4, count), F32),
            dma((3,)),
            dma((10,)),
            dma((1,)),
            dma((2, groups, 4)),
            dma((2, groups, 4, 2)),
            dma((2, groups)),
            dma((1,)),
            dma((1,)),
            dma((2, groups)),
            dma((2, groups, 4, 2)),
            dma((2, groups)),
            dma((1,)),
        ],
        compiler_params=pltpu.CompilerParams(
            collective_id=0, has_side_effects=True, vmem_limit_bytes=50 * 1024 * 1024
        ),
    )(hidden.reshape(groups, width), head_weight.reshape(4, quarter, columns), teacher)
    loss, hgrad, head_grad = pl.pallas_call(
        place_kernel,
        name="place_results",
        out_shape=(
            jax.ShapeDtypeStruct((1, groups), F32),
            jax.ShapeDtypeStruct((groups, width), BF16),
            jax.ShapeDtypeStruct((width, columns), BF16),
        ),
        in_specs=[vmem, vmem, vmem],
        out_specs=(any_space, any_space, any_space),
        scratch_shapes=[dma((3,))],
        compiler_params=pltpu.CompilerParams(vmem_limit_bytes=1024 * 1024),
    )(*(pltpu.with_memory_space_constraint(result, pltpu.VMEM) for result in results))
    return (loss.reshape(groups, 1), hgrad.reshape(groups, 1, width), head_grad)


def solution(mesh):
    split = Mesh(mesh.devices.reshape(NX, NY, NZ, NC), AXES)
    return jax.shard_map(
        shards,
        mesh=split,
        in_specs=(P(None, AXES, None), P(None, AXES), P(None, None, AXES)),
        out_specs=(P(None, AXES), P(None, AXES, None), P(None, AXES)),
        check_vma=False,
    )
```

```python
import jax
import jax.numpy as jnp
from jax import lax
from jax.experimental import pallas as pl
from jax.experimental.pallas import tpu as pltpu
from jax.sharding import Mesh
from jax.sharding import PartitionSpec as P

AXES = ("x", "y", "z", "c")
NX, NY, NZ, NC = 4, 4, 8, 2
LINE = NZ * NC
PLANE = NX * NY
BF16, F32 = jnp.bfloat16, jnp.float32
MESH = pl.DeviceIdType.MESH
RING = (2, 1, 3, 0)
FAR_PLANE = (10, 5, 7, 15, 13, 8, 2, 9, 11, 14, 6, 3, 1, 12, 4)
FAR_LINE = (8, 7, 9, 6, 10, 5, 11, 4, 12, 3, 13, 2, 14, 1, 15)


def main_kernel(
    hidden_ref, head_ref, teacher_ref, loss_ref, hgrad_ref, head_grad_ref,
    tokens, own, landed, spread, hid, head, teach, logit, grad, raised, raised_share, teach_share, weight, column, half_out, half_in,
    ring_out, ring_in, side_out, side_in, line_out, line_in,
    stat_out, stat_line, stat_mid, stat_plane, stat_all,
    local_sem, sent, p1_r, d1_r, d2_r, d2_l, pair_r, sl_r, sp_r, hp_r, rr_r, rd_r, zl_r,
):
    me = {a: lax.axis_index(a) for a in AXES}
    core = me["c"]
    other = 1 - core
    sign = 1 - 2 * core
    rank = me["z"] * NC + core
    place = me["x"] * NY + me["y"]
    width = hidden_ref.shape[1]
    half = width // 2
    quarter = half // 2
    groups, per, columns = teacher_ref.shape
    first, second = ("x", "y"), ("y", "x")

    def send(src, dst, ssem, rsem, where):
        copy = pltpu.make_async_remote_copy(
            src_ref=src, dst_ref=dst, send_sem=ssem, recv_sem=rsem, device_id=where, device_id_type=MESH
        )
        copy.start()
        return copy

    def wait_all(ref, sem):
        pltpu.make_async_copy(ref, ref, sem).wait()

    def line_peer(step):
        peer = lax.rem(rank + step, LINE)
        return peer, {"z": peer // NC, "c": lax.rem(peer, NC)}

    def plane_peer(step):
        peer = lax.rem(place + step, PLANE)
        return peer, {"x": peer // NY, "y": lax.rem(peer, NY)}

    def along(axis, step):
        return lax.rem(me[axis] + step + 4, 4)

    def masses(g):
        mass = jnp.sum(teach[g].astype(F32), axis=1, keepdims=True)
        weight[g] = jnp.broadcast_to(mass, weight.shape[1:])

    def product(ref, g, q):
        return lax.dot_general(
            ref[g], head[q], (((1,), (1,)), ((), ())), preferred_element_type=F32
        ).reshape(NX, NY, LINE, quarter)

    def share_teacher(g, q):
        teach_share[q, g] = product(teach, g, q)

    local = [
        pltpu.make_async_copy(hidden_ref, tokens, local_sem.at[0]),
        pltpu.make_async_copy(head_ref, head, local_sem.at[1]),
        pltpu.make_async_copy(teacher_ref, teach, local_sem.at[2]),
    ]
    for copy in local:
        copy.start()

    barrier = pltpu.get_barrier_semaphore()
    for step in FAR_LINE:
        _, where = line_peer(step)
        pl.semaphore_signal(barrier, inc=1, device_id=where, device_id_type=MESH)
    for step in FAR_PLANE:
        _, where = plane_peer(step)
        for c in (core, other):
            pl.semaphore_signal(barrier, inc=1, device_id={**where, "c": c}, device_id_type=MESH)

    local[0].wait()
    mine = tokens[...]
    for c in range(NC):
        own[c] = mine[:, c * half : (c + 1) * half]
    landed[rank] = own[core]
    pl.semaphore_wait(barrier, LINE - 1 + NC * (PLANE - 1))

    for step in FAR_LINE:
        peer, where = line_peer(step)
        send(own.at[where["c"]], landed.at[rank], sent.at[0], p1_r.at[0], where)
    for copy in local[1:]:
        copy.wait()
    masses(0)
    masses(1)
    share_teacher(0, 0)
    share_teacher(0, 1)
    share_teacher(0, 2)
    share_teacher(0, 3)
    share_teacher(1, 0)
    wait_all(landed.at[: LINE - 1], p1_r.at[0])
    for j in range(LINE):
        pair = landed[j].astype(F32)
        for g in range(groups):
            spread[g, j : j + 1] = pair[g : g + 1]
    for k in range(2):
        hid[2 * core + k, :, me["x"], me["y"]] = spread[:, :, k * quarter : (k + 1) * quarter].astype(BF16)

    direct, ring = {}, {}
    behind = (0, 1, 3, 2)

    def block(k, g, i1, i2):
        i = (i1, i2) if k == 0 else (i2, i1)
        return hid.at[2 * core + k, g, i[0], i[1]]

    def gather_first(g):
        for k in range(2):
            mine = block(k, g, me[first[k]], me[second[k]])
            for n in (1, 2, 3):
                direct[k, g, n] = send(
                    mine, mine, sent.at[1], d1_r.at[k, g, n - 1], {first[k]: along(first[k], behind[n])}
                )

    def gather_ring(g, order, d):
        for n in order:
            for k in range(2):
                if n and d == 0:
                    direct[k, g, n].wait_recv()
                column = block(k, g, along(first[k], -behind[n]), me[second[k]])
                ring[k, g, n, d] = send(
                    column, column, sent.at[2], d2_l.at[g, n] if d else d2_r.at[k, g, n],
                    {second[k]: along(second[k], sign * (1 - 2 * d))},
                )

    def gather_relay(g):
        for n in range(4):
            for k in range(2):
                ring[k, g, n, 0].wait_recv()
                column = block(k, g, along(first[k], -behind[n]), along(second[k], -sign))
                send(column, column, sent.at[2], d2_l.at[g, n], {second[k]: along(second[k], sign)})

    def gather_last(g):
        for n in range(4):
            wait_all(ring_in.at[:, g, n, :2], d2_l.at[g, n])
            for k in range(2):
                i1 = along(first[k], -behind[n])
                column = hid.at[2 * core + k, g, i1] if k == 0 else hid.at[2 * core + k, g, :, i1]
                send(column, column, sent.at[3], pair_r.at[k, g], {"c": other})

    def states(q, g):
        return hid[q, g].reshape(per, quarter)

    def add_quarter(g, q, fresh):
        here = slice(g * per, (g + 1) * per)
        for n in range(columns // 256):
            cols = slice(n * 256, (n + 1) * 256)
            term = jnp.dot(states(q, g), head[q, :, cols], preferred_element_type=F32)
            logit[here, cols] = term if fresh else logit[here, cols] + term

    def logits_own(g):
        for k in range(2):
            add_quarter(g, 2 * core + k, k == 0)

    def logits_other(g):
        for k in range(2):
            wait_all(hid.at[0, g], pair_r.at[k, g])
            add_quarter(g, 2 * other + k, False)

    def statistics():
        lane = lax.broadcasted_iota(jnp.int32, (per, 128), 1)
        for g in range(groups):
            part = logit[g * per : (g + 1) * per]
            wide = teach[g].astype(F32)
            peak = jnp.max(part, axis=1, keepdims=True)
            total = jnp.sum(jnp.exp(part - peak), axis=1, keepdims=True)
            mass = weight[g, :, 0:1]
            cross = jnp.sum(wide * part, axis=1, keepdims=True)
            packed = jnp.where(lane == 0, peak, jnp.where(lane == 1, total, jnp.where(lane == 2, mass, cross)))
            column[g] = jnp.broadcast_to(peak, (per, 128))
            stat_out[g] = packed.T[:4]
        stat_line[rank] = stat_out[core]
        for step in FAR_LINE:
            peer, where = line_peer(step)
            send(stat_out.at[where["c"]], stat_line.at[rank], sent.at[4], sl_r.at[0], where)

    def combined(ref, slots):
        every = [ref[j] for j in slots]
        peak = every[0][0:1]
        for one in every[1:]:
            peak = jnp.maximum(peak, one[0:1])
        total = sum(one[1:2] * jnp.exp(one[0:1] - peak) for one in every)
        mass = sum(one[2:3] for one in every)
        cross = sum(one[3:4] for one in every)
        return peak, total, mass, cross

    def line_done():
        wait_all(stat_line.at[: LINE - 1], sl_r.at[0])
        stat_mid[...] = jnp.concatenate(combined(stat_line, range(LINE)), axis=0)
        slot = core * PLANE + place
        stat_plane[slot] = stat_mid[...]
        for step in (*FAR_PLANE, 0):
            _, where = plane_peer(step)
            for c in (core, other) if step else (other,):
                send(stat_mid, stat_plane.at[slot], sent.at[5], sp_r.at[0], {**where, "c": c})

    def plane_done():
        wait_all(stat_plane.at[: NC * PLANE - 1], sp_r.at[0])
        for g in range(groups):
            peak, total, mass, cross = combined(stat_plane, range(g * PLANE, (g + 1) * PLANE))
            norm = peak + jnp.log(total)
            stat_all[g] = jnp.concatenate([norm, mass, mass * norm - cross, peak], axis=0)

    def scales(g):
        final = stat_all[g]
        token = lax.broadcasted_iota(jnp.int32, (1, per), 1)
        loss = jnp.sum(jnp.where(token == place * LINE + rank, final[2:3], 0.0), axis=1, keepdims=True)
        loss_ref[:, g : g + 1] = loss
        tall = jnp.concatenate([final, jnp.zeros((124, per), F32)], axis=0).T
        peak = column[g, :, 0:1]
        lane = lax.broadcasted_iota(jnp.int32, (per, 128), 1)
        scale = tall[:, 1:2] * jnp.exp(peak - tall[:, 0:1])
        column[g] = jnp.where(lane == 0, tall[:, 0:1], jnp.where(lane == 1, tall[:, 1:2], scale))

    def gradient(g):
        tall = column[g]
        part = logit[g * per : (g + 1) * per]
        grad[g] = (tall[:, 1:2] * jnp.exp(part - tall[:, 0:1]) - teach[g].astype(F32)).astype(BF16)

    over = {}

    def raise_group(g):
        part = logit[g * per : (g + 1) * per]
        raised[g] = jnp.exp(part - column[g, :, 0:1]).astype(BF16)

    def share_raised(g, q):
        raised_share[q, g] = product(raised, g, q)

    def joined(g, q):
        scale = column[g, :, 2:3].reshape(NX, NY, LINE, 1)
        return raised_share[q, g] * scale - teach_share[q, g]

    def share_over(g, k):
        q = 2 * other + k
        half_out[k, g] = joined(g, q).astype(BF16)
        over[k, g] = send(half_out.at[k, g], half_in.at[k, g], sent.at[6], hp_r.at[k, g], {"c": other})

    def share_kept(g, k):
        q = 2 * core + k
        raised_share[q, g] = joined(g, q)

    hop = {}

    def mine_at(k, g, i1, i2):
        i = (i1, i2) if k == 0 else (i2, i1)
        return raised_share[2 * core + k, g, i[0], i[1]] + half_in[k, g, i[0], i[1]].astype(F32)

    def push(k, g, r, d, value, step):
        ring_out[k, g, r, d] = value.astype(BF16)
        hop[k, g, r, d] = send(
            ring_out.at[k, g, r, d], ring_in.at[k, g, r, d], sent.at[7], rr_r.at[k, g, r, min(d, 1)],
            {second[k]: along(second[k], step)},
        )

    def sum_start(g, k, d):
        if d == 0:
            over[k, g].wait_recv()
        for r in RING:
            i1 = along(first[k], r)
            push(k, g, r, d, mine_at(k, g, i1, along(second[k], -sign if d else 2)), -sign if d else sign)

    def sum_relay(g, k):
        for r in RING:
            i1 = along(first[k], r)
            hop[k, g, r, 0].wait_recv()
            carried = ring_in[k, g, r, 0].astype(F32)
            push(k, g, r, 2, mine_at(k, g, i1, along(second[k], sign)) + carried, sign)

    def sum_last(g, k):
        for r in RING:
            i1 = along(first[k], r)
            wait_all(ring_in.at[k, g, r, 1:], rr_r.at[k, g, r, 1])
            total = mine_at(k, g, i1, me[second[k]])
            total = total + ring_in[k, g, r, 1].astype(F32) + ring_in[k, g, r, 2].astype(F32)
            if r:
                side_out[k, g, r] = total.astype(BF16)
                send(side_out.at[k, g, r], side_in.at[k, g, r], sent.at[8], rd_r.at[k, g], {first[k]: i1})
            else:
                spread[g, :, k * quarter : (k + 1) * quarter] = total

    def sum_side(g):
        for k in range(2):
            here = slice(k * quarter, (k + 1) * quarter)
            total = spread[g, :, here]
            wait_all(side_in.at[k, g, 1:], rd_r.at[k, g])
            for r in RING[:3]:
                total = total + side_in[k, g, r].astype(F32)
            spread[g, :, here] = total

    def head_gradient(q):
        head_grad_ref[q * quarter : (q + 1) * quarter] = lax.dot_general(
            hid[q].reshape(groups * per, quarter), grad[...].reshape(groups * per, columns),
            (((0,), (0,)), ((), ())), preferred_element_type=F32,
        ).astype(BF16)

    gather_first(0)
    gather_ring(0, (0,), 0)
    gather_ring(0, (0,), 1)
    gather_first(1)
    share_teacher(1, 1)
    share_teacher(1, 2)
    gather_ring(0, (1, 2, 3), 0)
    gather_ring(0, (1, 2, 3), 1)
    gather_ring(1, (0, 1, 2, 3), 0)
    gather_ring(1, (0, 1, 2, 3), 1)
    share_teacher(1, 3)
    gather_relay(0)
    gather_relay(1)
    gather_last(0)
    logits_own(0)
    gather_last(1)
    logits_own(1)
    logits_other(0)
    logits_other(1)
    statistics()
    raise_group(0)
    share_raised(0, 2 * other)
    share_raised(0, 2 * core)
    share_raised(0, 2 * other + 1)
    share_raised(0, 2 * core + 1)
    line_done()
    raise_group(1)
    share_raised(1, 2 * other)
    share_raised(1, 2 * core)
    share_raised(1, 2 * other + 1)
    share_raised(1, 2 * core + 1)
    plane_done()
    scales(0)
    share_over(0, 0)
    share_over(0, 1)
    scales(1)
    share_over(1, 0)
    share_over(1, 1)
    share_kept(0, 0)
    sum_start(0, 0, 0)
    share_kept(0, 1)
    sum_start(0, 1, 0)
    share_kept(1, 0)
    sum_start(1, 0, 0)
    share_kept(1, 1)
    sum_start(1, 1, 0)
    sum_start(0, 0, 1)
    sum_start(0, 1, 1)
    sum_relay(0, 0)
    sum_relay(0, 1)
    sum_start(1, 0, 1)
    sum_start(1, 1, 1)
    sum_relay(1, 0)
    sum_relay(1, 1)
    gradient(0)
    gradient(1)
    sum_last(0, 0)
    sum_last(0, 1)
    sum_last(1, 0)
    sum_last(1, 1)
    sum_side(0)
    sum_side(1)
    for j in range(LINE):
        line_out[j] = jnp.concatenate([spread[g, j : j + 1] for g in range(groups)], axis=0).astype(BF16)
    line_in[core, me["z"]] = line_out[rank]
    for step in FAR_LINE:
        peer, where = line_peer(step)
        send(line_out.at[peer], line_in.at[core, me["z"]], sent.at[9], zl_r.at[0], where)
    head_gradient(0)
    head_gradient(1)
    head_gradient(2)
    head_gradient(3)
    wait_all(line_out.at[: LINE - 1], zl_r.at[0])
    for c in range(NC):
        total = line_in[c, 0].astype(F32)
        for z in range(1, NZ):
            total = total + line_in[c, z].astype(F32)
        hgrad_ref[:, c * half : (c + 1) * half] = total.astype(BF16)

    for n, ref in enumerate(
        (
            landed.at[: LINE - 1], ring_in.at[:, :, 0], ring_in, hid.at[:2], stat_line.at[: LINE - 1],
            stat_plane.at[: NC * PLANE - 1], half_out, ring_out, side_out.at[:, :, 1:],
            line_out.at[: LINE - 1],
        )
    ):
        wait_all(ref, sent.at[n])


def place_kernel(loss_in, hgrad_in, head_in, loss_ref, hgrad_ref, head_ref, sem):
    copies = [
        pltpu.make_async_copy(head_in, head_ref, sem.at[0]),
        pltpu.make_async_copy(hgrad_in, hgrad_ref, sem.at[1]),
        pltpu.make_async_copy(loss_in, loss_ref, sem.at[2]),
    ]
    for copy in copies:
        copy.start()
    for copy in copies:
        copy.wait()


def shards(hidden, head_weight, teacher):
    groups, _, width = hidden.shape
    columns = head_weight.shape[1]
    count = teacher.shape[1]
    half, quarter = width // 2, width // 4
    plane = (groups, NX, NY, LINE, quarter)
    block = (LINE, quarter)
    dma = pltpu.SemaphoreType.DMA
    vmem = pl.BlockSpec(memory_space=pltpu.VMEM)
    any_space = pl.BlockSpec(memory_space=pl.ANY)
    results = pl.pallas_call(
        main_kernel,
        name="gather_loss_reduce",
        out_shape=(
            pltpu.VMEM((1, groups), F32),
            pltpu.VMEM((groups, width), BF16),
            pltpu.VMEM((width, columns), BF16),
        ),
        in_specs=[any_space, any_space, any_space],
        out_specs=(vmem, vmem, vmem),
        scratch_shapes=[
            pltpu.VMEM((groups, width), BF16),
            pltpu.VMEM((NC, groups, half), BF16),
            pltpu.VMEM((LINE, groups, half), BF16),
            pltpu.VMEM((groups, LINE, half), F32),
            pltpu.VMEM((4, *plane), BF16),
            pltpu.VMEM((4, quarter, columns), BF16),
            pltpu.VMEM((groups, count, columns), BF16),
            pltpu.VMEM((groups * count, columns), F32),
            pltpu.VMEM((groups, count, columns), BF16),
            pltpu.VMEM((groups, count, columns), BF16),
            pltpu.VMEM((4, *plane), F32),
            pltpu.VMEM((4, *plane), F32),
            pltpu.VMEM((groups, count, 128), F32),
            pltpu.VMEM((groups, count, 128), F32),
            pltpu.VMEM((2, *plane), BF16),
            pltpu.VMEM((2, *plane), BF16),
            pltpu.VMEM((2, groups, 4, 3, *block), BF16),
            pltpu.VMEM((2, groups, 4, 3, *block), BF16),
            pltpu.VMEM((2, groups, 4, *block), BF16),
            pltpu.VMEM((2, groups, 4, *block), BF16),
            pltpu.VMEM((LINE, groups, half), BF16),
            pltpu.VMEM((NC, NZ, groups, half), BF16),
            pltpu.VMEM((groups, 4, count), F32),
            pltpu.VMEM((LINE, 4, count), F32),
            pltpu.VMEM((4, count), F32),
            pltpu.VMEM((NC * PLANE, 4, count), F32),
            pltpu.VMEM((groups, 4, count), F32),
            dma((3,)),
            dma((10,)),
            dma((1,)),
            dma((2, groups, 3)),
            dma((2, groups, 4)),
            dma((groups, 4)),
            dma((2, groups)),
            dma((1,)),
            dma((1,)),
            dma((2, groups)),
            dma((2, groups, 4, 2)),
            dma((2, groups)),
            dma((1,)),
        ],
        compiler_params=pltpu.CompilerParams(
            collective_id=0, has_side_effects=True, vmem_limit_bytes=50 * 1024 * 1024
        ),
    )(hidden.reshape(groups, width), head_weight.reshape(4, quarter, columns), teacher)
    loss, hgrad, head_grad = pl.pallas_call(
        place_kernel,
        name="place_results",
        out_shape=(
            jax.ShapeDtypeStruct((1, groups), F32),
            jax.ShapeDtypeStruct((groups, width), BF16),
            jax.ShapeDtypeStruct((width, columns), BF16),
        ),
        in_specs=[vmem, vmem, vmem],
        out_specs=(any_space, any_space, any_space),
        scratch_shapes=[dma((3,))],
        compiler_params=pltpu.CompilerParams(vmem_limit_bytes=1024 * 1024),
    )(*(pltpu.with_memory_space_constraint(result, pltpu.VMEM) for result in results))
    return (loss.reshape(groups, 1), hgrad.reshape(groups, 1, width), head_grad)


def solution(mesh):
    split = Mesh(mesh.devices.reshape(NX, NY, NZ, NC), AXES)
    return jax.shard_map(
        shards,
        mesh=split,
        in_specs=(P(None, AXES, None), P(None, AXES), P(None, None, AXES)),
        out_specs=(P(None, AXES), P(None, AXES, None), P(None, AXES)),
        check_vma=False,
    )
```
